128 devices in a mesh: seq: 16 (over y, x), head: 8 (over z, core).
Axes of the slice: x: 4, y: 4, z: 4, core: 2. Of those that a mesh axis runs over, the one named last changes fastest.
Arguments:
- queries: bfloat16 [4096, 16384], P('seq', 'head'), may hold values from -6 to 6
- keys: bfloat16 [4096, 1024], P('seq', 'head'), may hold values from -6 to 6
- values: bfloat16 [4096, 1024], P('seq', 'head'), may hold values from -6 to 6
- teacher: bfloat16 [4096, 16384], P('seq', 'head'), may hold values from -17 to 17
- map_q: bfloat16 [128, 128, 64], P('head'), may hold values from -0.5 to 0.5
- map_k: bfloat16 [128, 128, 64], P('head'), may hold values from -0.5 to 0.5
Outputs:
- grad_map_q: float32 [128, 128, 64], P('head', 'seq')
- grad_map_k: float32 [128, 128, 64], P('head', 'seq')
The draws below stay inside these ranges and needn't reach their ends.
All inputs are finite; a program needn't handle non-finite values.
Results may differ from the reference program's by a relative error of at most 0.0003.
Values sent between devices are 32-bit elements; how exact they have to be, the bound alone decides.
A program may use at most 128 MiB of HBM per device.

```python
import jax
import jax.numpy as jnp
from jax import lax

HEADS = 128
KV_HEADS = 8
DH = 128
FH = 64
BLOCK = 256
SEQ = 4096


def draw_teacher(key, part):
    row_count = SEQ
    col_count = HEADS * DH
    head_pos = (jnp.arange(col_count, dtype=jnp.int32) // DH).astype(jnp.float32)
    rising = 1.0 + 2.0 * head_pos / max(HEADS - 1, 1)
    base = jax.random.truncated_normal(jax.random.fold_in(key, 5), -4.0, 4.0, (row_count, col_count), jnp.float32)
    return (base * rising[None, :]).astype(jnp.bfloat16)


def level_of(stream_key, extent, split, smallest, top_value):
    gain, own = 1.0, jax.random.fold_in(stream_key, 6)
    for dim, blocks in split:
        draws = jnp.exp(jax.random.uniform(jax.random.fold_in(own, dim), (blocks,), jnp.float32, smallest / len(split), top_value / len(split)))
        gain = gain * jnp.repeat(draws, extent[dim] // blocks).reshape([-1 if axis == dim else 1 for axis in range(len(extent))])
    return gain


def bell_draw(stream_key, extent, scale, bound, pieces=(), kind=jnp.bfloat16):
    values = scale * jax.random.normal(stream_key, extent, jnp.float32)
    if pieces:
        values = values * level_of(stream_key, extent, pieces, -0.22, 0.18)
    return jnp.clip(values, -bound, bound).astype(kind)


def setup_inputs(seed: int = 0) -> dict:
    key_list = jax.random.split(jax.random.key(seed), 7)
    return {
        "queries": bell_draw(key_list[0], (SEQ, HEADS * DH), 1.0, 6.0, ((0, 16), (1, 8))),
        "keys": bell_draw(key_list[1], (SEQ, KV_HEADS * DH), 1.0, 6.0, ((0, 16), (1, 8))),
        "values": bell_draw(key_list[2], (SEQ, KV_HEADS * DH), 1.0, 6.0, ((0, 16), (1, 8))),
        "teacher": draw_teacher(jax.random.fold_in(key_list[6], 71), 0),
        "map_q": bell_draw(key_list[4], (HEADS, DH, FH), DH ** -0.5, 0.5, ((0, 8),)),
        "map_k": bell_draw(key_list[5], (HEADS, DH, FH), DH ** -0.5, 0.5, ((0, 8),)),
    }


exact_mode = lax.Precision.HIGHEST

def features(inputs, weight):
    logits = jnp.dot(inputs.astype(jnp.float32), weight, precision=exact_mode)
    positive = jnp.exp(logits)
    negative = jnp.exp(-logits)
    return jnp.concatenate([positive / lax.optimization_barrier(jnp.sum(positive, -1, keepdims=True)), negative / lax.optimization_barrier(jnp.sum(negative, -1, keepdims=True))], -1)

def head_loss(w_query, w_key, queries, keys, values, teacher, power):
    query_feat = features(queries, w_query)
    key_feat = features(keys, w_key)
    block_count = queries.shape[0] // BLOCK
    causal = jnp.tril(jnp.ones((BLOCK, BLOCK), jnp.float32))

    def step(carried, blocks):
        kv_state, key_total = carried
        q_blk, k_blk, v_blk, t_blk, p_blk = blocks
        scores = jnp.dot(q_blk, k_blk.T, precision=exact_mode) * causal
        numerator = jnp.dot(q_blk, kv_state, precision=exact_mode) + jnp.dot(scores, v_blk, precision=exact_mode)
        denominator = jnp.dot(q_blk, key_total, precision=exact_mode) + lax.optimization_barrier(jnp.sum(scores, -1))
        student = numerator / denominator[:, None]
        error = student - t_blk
        partial_loss = 0.5 * jnp.sum(error * error / p_blk[:, None])
        new_state = kv_state + jnp.dot(k_blk.T, v_blk, precision=exact_mode)
        return ((new_state, key_total + lax.optimization_barrier(jnp.sum(k_blk, 0))), partial_loss)
    feat_width = query_feat.shape[1]
    start = (jnp.zeros((feat_width, DH), jnp.float32), jnp.zeros((feat_width,), jnp.float32))
    blocks = (query_feat.reshape(block_count, BLOCK, feat_width), key_feat.reshape(block_count, BLOCK, feat_width), values.astype(jnp.float32).reshape(block_count, BLOCK, DH), teacher.astype(jnp.float32).reshape(block_count, BLOCK, DH), power.reshape(block_count, BLOCK))
    _, partials = lax.scan(step, start, blocks)
    return jnp.sum(partials)

def reference(queries, keys, values, teacher, map_q, map_k):
    power = lax.optimization_barrier(jnp.sum(jnp.square(teacher.astype(jnp.float32)), axis=1)) / (HEADS * DH) + 1e-05
    group_size = HEADS // KV_HEADS

    def one_head(head_idx):
        offset = (head_idx * DH).astype(jnp.int32)
        shared = (head_idx // group_size * DH).astype(jnp.int32)

        def take_head(source):
            return lax.dynamic_slice_in_dim(source, offset, DH, 1)

        def take_shared(source):
            return lax.dynamic_slice_in_dim(source, shared, DH, 1)
        return jax.grad(head_loss, argnums=(0, 1))(map_q[head_idx].astype(jnp.float32), map_k[head_idx].astype(jnp.float32), take_head(queries), take_shared(keys), take_shared(values), take_head(teacher), power)
    grad_q, grad_k = lax.map(one_head, jnp.arange(HEADS, dtype=jnp.int32))
    return (grad_q, grad_k)
```

```python
import functools

import jax
import jax.numpy as jnp
from jax import lax
from jax.experimental import pallas as pl
from jax.experimental.pallas import tpu as pltpu
from jax.sharding import PartitionSpec as P

HEADS = 128
DH = 128
FH = 64
T = 256
NS = 16
NH = 8
ROWS = 136
MESH = pl.DeviceIdType.MESH
F32 = jnp.float32
BF16 = jnp.bfloat16


def split(x):
    high = x.astype(BF16)
    return high, (x - high.astype(F32)).astype(BF16)


def cols(x, y):
    return jnp.concatenate([x, y], axis=1)


def dot(a, b):
    return jnp.dot(a, b, preferred_element_type=F32)


def dot_t(a, b):
    return lax.dot_general(a, b, (((1,), (1,)), ((), ())), preferred_element_type=F32)


def fold(x):
    return x[:, :128] + x[:, 128:]


def kernel(
    q, k, v, t, mq, mk, oq, ok,
    khl, qhl, ghl, ni, dp, gd_s, rp, vta, vv, kt_s, bb,
    p_send, p_recv, a_send, a_recv, c_send, c_recv, d_send, d_recv, f_send, f_recv,
    gq_send, gq_recv, gk_send, gk_recv,
    ss, rs, pss, prs,
):
    me = lax.axis_index("seq")
    hd = lax.axis_index("head")

    barrier = pltpu.get_barrier_semaphore()
    for j in range(1, NS):
        pl.semaphore_signal(
            barrier, inc=1, device_id={"seq": lax.rem(me + j, NS)}, device_id_type=MESH
        )
    for j in range(1, NH):
        pl.semaphore_signal(
            barrier, inc=1, device_id={"head": lax.rem(hd + j, NH)}, device_id_type=MESH
        )

    def seq_copy(phase, src, dst_buf, dst, slot):
        return pltpu.make_async_remote_copy(
            src_ref=src,
            dst_ref=dst_buf.at[slot],
            send_sem=ss.at[phase, dst],
            recv_sem=rs.at[phase, slot],
            device_id={"seq": dst},
            device_id_type=MESH,
        )

    def arrived(phase, buf, slot):
        pltpu.make_async_remote_copy(
            src_ref=buf.at[slot],
            dst_ref=buf.at[slot],
            send_sem=ss.at[phase, slot],
            recv_sem=rs.at[phase, slot],
            device_id={"seq": slot},
            device_id_type=MESH,
        ).wait_recv()

    def power_copy(dst, slot):
        return pltpu.make_async_remote_copy(
            src_ref=p_send,
            dst_ref=p_recv.at[slot],
            send_sem=pss.at[dst],
            recv_sem=prs.at[slot],
            device_id={"head": dst},
            device_id_type=MESH,
        )

    def head_cols(ref, h):
        return ref[:, pl.ds(pl.multiple_of(h * DH, DH), DH)]

    row = lax.broadcasted_iota(jnp.int32, (2 * DH, DH), 0)
    col = lax.broadcasted_iota(jnp.int32, (2 * DH, DH), 1)
    bb[...] = jnp.where(lax.rem(row, DH) // FH == col // FH, 1.0, 0.0).astype(BF16)
    causal = lax.broadcasted_iota(jnp.int32, (T, T), 0) >= lax.broadcasted_iota(
        jnp.int32, (T, T), 1
    )
    vta[:DH] = v[...].T
    vta[DH:] = jnp.ones((16, T), BF16)
    vv[...] = cols(v[...], v[...])
    kt_s[...] = k[...].T

    def seg_sum(x):
        return dot(cols(*split(x)), bb[...])

    def features(x, m):
        e = jnp.exp(dot(x, cols(m, -m)))
        return cols(*split(e * (1.0 / seg_sum(e))))

    def stage_a(j, _):
        h = lax.rem(me + 1 + j, NS)
        f = features(k[...], mk[h])
        khl[h] = f
        a_send[h] = fold(dot(vta[...], f))[:ROWS]

        @pl.when(j == 0)
        def _():
            pl.semaphore_wait(barrier, NS + NH - 2)

        @pl.when(j < NS - 1)
        def _():
            seq_copy(0, a_send.at[h], a_recv, h, me).start()

        return 0

    lax.fori_loop(0, NS, stage_a, 0)
    a_recv[me] = a_send[me]

    def squares(j, total):
        x = head_cols(t, j).astype(F32)
        return total + x * x

    sq = lax.fori_loop(0, NS, squares, jnp.zeros((T, DH), F32))
    p_send[...] = jnp.broadcast_to(jnp.sum(sq.T, axis=0, keepdims=True), (8, T))
    for j in range(1, NH):
        power_copy(lax.rem(hd + j, NH), hd).start()

    def stage_b(h, _):
        f = features(head_cols(q, h), mq[h])
        qhl[h] = f
        g = khl[h]
        gh = g[:, :DH]
        s = dot_t(f, cols(gh, gh)) + dot_t(f[:, :DH], g[:, DH:])
        s = jnp.where(causal, s, 0.0)
        sh, sl = split(s)
        ni[h] = dot(sh, v[...]) + dot(sl, v[...])
        dp[h] = fold(s)
        return 0

    lax.fori_loop(0, NS, stage_b, 0)

    def stage_c(s, total):
        @pl.when(s != me)
        def _():
            arrived(0, a_recv, s)

        c_send[s] = total
        return total + a_recv[s]

    lax.fori_loop(0, NS, stage_c, jnp.zeros((ROWS, DH), F32))

    def send_c(j, _):
        dst = lax.rem(me + j, NS)
        seq_copy(1, c_send.at[dst], c_recv, dst, me).start()
        return 0

    lax.fori_loop(1, NS, send_c, 0)
    c_recv[me] = c_send[me]

    power = p_send[...]
    for j in range(1, NH):
        power_copy(lax.rem(hd + j, NH), lax.rem(hd + j, NH)).wait_recv()
        power = power + p_recv[lax.rem(hd + j, NH)]
    power = power / (HEADS * DH) + 1e-05
    rp[...] = jnp.broadcast_to((1.0 / power).T[:, :1], (T, DH))

    def stage_d(j, _):
        h = lax.rem(me - j + NS, NS)

        @pl.when(j > 0)
        def _():
            arrived(1, c_recv, h)

        sh, sl = split(c_recv[h, :DH])
        key_total = c_recv[h, DH : DH + 1]
        f = qhl[h]
        w = jnp.concatenate([cols(sh, sh), cols(sl, sl)], axis=0)
        numer = ni[h] + fold(dot_t(f, w))
        qf = f[:, :DH].astype(F32) + f[:, DH:].astype(F32)
        den = jnp.sum(dp[h] + qf * key_total, axis=1, keepdims=True)
        rden = 1.0 / den
        student = numer * rden
        gn = (student - head_cols(t, h).astype(F32)) * rp[...] * rden
        gd = -jnp.sum(gn * student, axis=1, keepdims=True)
        ghl[h] = cols(*split(gn))
        gd_s[h] = jnp.broadcast_to(gd, (T, DH))
        th, tl = split(gn.T)
        d_send[h, :DH] = fold(dot(th, f) + dot(tl, f))
        d_send[h, DH:] = jnp.broadcast_to(jnp.sum(qf * gd, axis=0, keepdims=True), (8, DH))

        @pl.when(j > 0)
        def _():
            seq_copy(2, d_send.at[h], d_recv, h, me).start()

        return 0

    lax.fori_loop(0, NS, stage_d, 0)
    d_recv[me] = d_send[me]

    def map_grad(xt, feat, grad):
        r = feat * (grad - seg_sum(feat * grad))
        y = fold(dot(xt, cols(*split(r))))
        return (y[:, :FH] - y[:, FH:]).reshape(NS, 8, FH)

    def put(buf, h, g):
        @pl.when(lax.rem(h, 2) == 0)
        def _():
            buf[:, h // 2, :, :FH] = g

        @pl.when(lax.rem(h, 2) == 1)
        def _():
            buf[:, h // 2, :, FH:] = g

    def stage_e(h, _):
        g = ghl[h]
        gd = gd_s[h]
        f = qhl[h]
        b = jnp.where(causal, dot_t(g, vv[...]) + cols(gd, gd), 0.0)
        bh, bl = split(b)
        s = cols(*split(c_recv[h, :DH]))
        kf = khl[h]
        o = dot(bh, kf) + dot(bl, kf) + dot(g, jnp.concatenate([s, s], axis=0))
        grad = fold(o) + gd * c_recv[h, DH : DH + 1]
        qf = f[:, :DH].astype(F32) + f[:, DH:].astype(F32)
        put(gq_send, h, map_grad(head_cols(q, h).T, qf, grad))
        ni[h] = fold(dot(bh.T, f) + dot(bl.T, f))
        return 0

    lax.fori_loop(0, NS, stage_e, 0)
    gq_recv[me] = gq_send[me]

    def stage_f(j, total):
        s = NS - 1 - j

        @pl.when(s != me)
        def _():
            arrived(2, d_recv, s)

        f_send[s] = total
        return total + d_recv[s]

    lax.fori_loop(0, NS, stage_f, jnp.zeros((ROWS, DH), F32))

    def send_f(j, _):
        dst = lax.rem(me + j, NS)
        seq_copy(3, f_send.at[dst], f_recv, dst, me).start()
        return 0

    lax.fori_loop(1, NS, send_f, 0)
    f_recv[me] = f_send[me]

    def send_gq(j, _):
        dst = lax.rem(me + j, NS)
        seq_copy(4, gq_send.at[dst], gq_recv, dst, me).start()
        return 0

    lax.fori_loop(1, NS, send_gq, 0)

    def stage_g(j, _):
        h = lax.rem(me - j + NS, NS)

        @pl.when(j > 0)
        def _():
            arrived(3, f_recv, h)

        s = cols(*split(f_recv[h, :DH]))
        grad = ni[h] + fold(dot(v[...], s)) + f_recv[h, DH : DH + 1]
        f = khl[h]
        kf = f[:, :DH].astype(F32) + f[:, DH:].astype(F32)
        put(gk_send, h, map_grad(kt_s[...], kf, grad))
        return 0

    lax.fori_loop(0, NS, stage_g, 0)
    gk_recv[me] = gk_send[me]

    def send_gk(j, _):
        dst = lax.rem(me + j, NS)
        seq_copy(5, gk_send.at[dst], gk_recv, dst, me).start()
        return 0

    lax.fori_loop(1, NS, send_gk, 0)

    def collect(phase, buf, out):
        def step(s, total):
            @pl.when(s != me)
            def _():
                arrived(phase, buf, s)

            return total + buf[s]

        total = lax.fori_loop(0, NS, step, jnp.zeros((NS // 2, 8, DH), F32))
        for p in range(NS // 2):
            out[2 * p] = total[p, :, :FH]
            out[2 * p + 1] = total[p, :, FH:]

    collect(4, gq_recv, oq)
    collect(5, gk_recv, ok)

    for phase, buf, dst_buf in (
        (0, a_send, a_recv),
        (1, c_send, c_recv),
        (2, d_send, d_recv),
        (3, f_send, f_recv),
        (4, gq_send, gq_recv),
        (5, gk_send, gk_recv),
    ):
        def drain(j, _, phase=phase, buf=buf, dst_buf=dst_buf):
            dst = lax.rem(me + j, NS)
            seq_copy(phase, buf.at[dst], dst_buf, dst, me).wait_send()
            return 0

        lax.fori_loop(1, NS, drain, 0)
    for j in range(1, NH):
        power_copy(lax.rem(hd + j, NH), hd).wait_send()


def on_device(queries, keys, values, teacher, map_q, map_k):
    state = pltpu.VMEM((NS, ROWS, DH), F32)
    share = pltpu.VMEM((NS, NS // 2, 8, DH), F32)
    pair = pltpu.VMEM((NS, T, 2 * DH), BF16)
    whole = pltpu.VMEM((NS, T, DH), F32)
    vmem = pl.BlockSpec(memory_space=pltpu.VMEM)
    out = jax.ShapeDtypeStruct((NS, 8, FH), F32)
    return pl.pallas_call(
        kernel,
        out_shape=(out, out),
        in_specs=[vmem] * 6,
        out_specs=(vmem, vmem),
        scratch_shapes=[
            pair, pair, pair,
            whole, whole, whole,
            pltpu.VMEM((T, DH), F32),
            pltpu.VMEM((DH + 16, T), BF16),
            pltpu.VMEM((T, 2 * DH), BF16),
            pltpu.VMEM((DH, T), BF16),
            pltpu.VMEM((2 * DH, DH), BF16),
            pltpu.VMEM((8, T), F32),
            pltpu.VMEM((NH, 8, T), F32),
            state, state, state, state, state, state, state, state,
            share, share, share, share,
            pltpu.SemaphoreType.DMA((6, NS)),
            pltpu.SemaphoreType.DMA((6, NS)),
            pltpu.SemaphoreType.DMA((NH,)),
            pltpu.SemaphoreType.DMA((NH,)),
        ],
        compiler_params=pltpu.CompilerParams(
            collective_id=0, has_side_effects=True, vmem_limit_bytes=56 * 2**20
        ),
    )(queries, keys, values, teacher, map_q, map_k)


def solution(mesh):
    placed = (
        P("seq", "head"),
        P("seq", "head"),
        P("seq", "head"),
        P("seq", "head"),
        P("head", None, None),
        P("head", None, None),
    )
    return jax.shard_map(
        on_device,
        mesh=mesh,
        in_specs=placed,
        out_specs=(P("head", "seq", None), P("head", "seq", None)),
        check_vma=False,
    )
```

```python
import jax
import jax.numpy as jnp
from jax import lax
from jax.experimental import pallas as pl
from jax.experimental.pallas import tpu as pltpu
from jax.sharding import PartitionSpec as P

HEADS = 128
DH = 128
FH = 64
T = 256
NS = 16
NH = 8
HALF = DH // 2
ROWS = HALF + 8
SENT = HALF + 1
NG = 2
PG = NS // NG
GA, GB, GD, GE, GG = 4, 2, 2, 2, 2
MESH = pl.DeviceIdType.MESH
F32 = jnp.float32
BF16 = jnp.bfloat16


def split(x):
    high = x.astype(BF16)
    return high, (x - high.astype(F32)).astype(BF16)


def cols(x, y):
    return jnp.concatenate([x, y], axis=1)


def dot(a, b):
    return jnp.dot(a, b, preferred_element_type=F32)


def dot_t(a, b):
    return lax.dot_general(a, b, (((1,), (1,)), ((), ())), preferred_element_type=F32)


def join(x):
    return x[:, :DH].astype(F32) + x[:, DH:].astype(F32)


def fold(x):
    return x[:, :128] + x[:, 128:]


def kernel(
    q, k, v, t, mq, mk, oq, ok,
    khl, qhl, ghl, ni, dp, gd_s, rp, vta, vv, bb,
    p_send, p_recv, a_send, a_recv, c_send, c_recv, d_send, d_recv, f_send, f_recv,
    gq_send, gq_recv, gk_send, gk_recv, gk_sum,
    ss, rs, pss, prs,
):
    me = lax.axis_index("seq")
    hd = lax.axis_index("head")
    mine = me // 2
    sibling = me + 1 - 2 * lax.rem(me, 2)

    barrier = pltpu.get_barrier_semaphore()
    for j in range(1, NS):
        pl.semaphore_signal(
            barrier, inc=1, device_id={"seq": lax.rem(me + j, NS)}, device_id_type=MESH
        )
    for j in range(1, NH):
        pl.semaphore_signal(
            barrier, inc=1, device_id={"head": lax.rem(hd + j, NH)}, device_id_type=MESH
        )

    def sent(buf, g, slot):
        if buf.shape[2] == ROWS:
            return buf.at[g, slot, pl.ds(0, SENT)]
        return buf.at[g, slot]

    def seq_copy(phase, g, buf, dst_buf, dst):
        return pltpu.make_async_remote_copy(
            src_ref=sent(buf, g, dst),
            dst_ref=sent(dst_buf, g, me),
            send_sem=ss.at[phase, g, dst],
            recv_sem=rs.at[phase, g, me],
            device_id={"seq": dst},
            device_id_type=MESH,
        )

    def arrived(phase, g, buf, slot):
        pltpu.make_async_remote_copy(
            src_ref=sent(buf, g, slot),
            dst_ref=sent(buf, g, slot),
            send_sem=ss.at[phase, g, slot],
            recv_sem=rs.at[phase, g, slot],
            device_id={"seq": slot},
            device_id_type=MESH,
        ).wait_recv()

    def send_all(phase, g, buf, dst_buf):
        def step(j, _):
            seq_copy(phase, g, buf, dst_buf, lax.rem(me + j, NS)).start()
            return 0

        lax.fori_loop(1, NS, step, 0)

    def owners(cs, own):
        return [2 * c + i for c in (cs[:-1] if own else cs) for i in range(2)] + (
            [sibling] if own else []
        )

    def states(buf, g, c):
        return jnp.concatenate([buf[g, 2 * c, :HALF], buf[g, 2 * c + 1, :HALF]], axis=0)

    def totals(buf, g, c):
        return buf[g, 2 * c, HALF:SENT]

    def power_copy(dst, slot):
        return pltpu.make_async_remote_copy(
            src_ref=p_send,
            dst_ref=p_recv.at[slot],
            send_sem=pss.at[dst],
            recv_sem=prs.at[slot],
            device_id={"head": dst},
            device_id_type=MESH,
        )

    def head_cols(ref, h):
        return ref[:, pl.ds(pl.multiple_of(h * DH, DH), DH)]

    even = lax.broadcasted_iota(jnp.int32, (DH, DH), 1) < FH

    row = lax.broadcasted_iota(jnp.int32, (2 * DH, DH), 0)
    col = lax.broadcasted_iota(jnp.int32, (2 * DH, DH), 1)
    bb[...] = jnp.where(lax.rem(row, DH) // FH == col // FH, 1.0, 0.0).astype(BF16)
    vta[:DH] = v[...].T
    vta[DH:] = jnp.ones((16, T), BF16)
    vv[...] = cols(v[...], v[...])

    tri = lax.broadcasted_iota(jnp.int32, (DH, DH), 0) >= lax.broadcasted_iota(
        jnp.int32, (DH, DH), 1
    )

    def seg_sum(x):
        return dot(cols(*split(x)), bb[...])

    def features(xs, ms):
        es = [jnp.exp(dot_t(x, jnp.concatenate([m, -m], axis=0))) for x, m in zip(xs, ms)]
        sums = [seg_sum(e) for e in es]
        return [cols(*split(e * (1.0 / z))) for e, z in zip(es, sums)]

    def stage_a(g, j0, own):
        cs = [lax.rem(mine + 1 + j0 + i, PG) for i in range(GA)]
        hs = [g * PG + c for c in cs]
        fs = features([k[...]] * GA, [mk[h] for h in hs])
        ps = [fold(dot(vta[...], f)) for f in fs]
        for c, h, f, p in zip(cs, hs, fs, ps):
            khl[h] = f
            a_send[g, 2 * c, :HALF] = p[:HALF]
            a_send[g, 2 * c + 1, :HALF] = p[HALF:DH]
            a_send[g, 2 * c, HALF:] = p[DH : DH + 8]
            a_send[g, 2 * c + 1, HALF:] = p[DH : DH + 8]
        return owners(cs, own)

    for g in range(NG):
        for j0 in range(0, PG, GA):
            dsts = stage_a(g, j0, j0 + GA == PG)
            if g == 0 and j0 == 0:
                pl.semaphore_wait(barrier, NS + NH - 2)
            for dst in dsts:
                seq_copy(0, g, a_send, a_recv, dst).start()
        a_recv[g, me] = a_send[g, me]

    def squares(j, total):
        x = head_cols(t, j).astype(F32)
        return total + x * x

    sq = lax.fori_loop(0, NS, squares, jnp.zeros((T, DH), F32))
    p_send[...] = jnp.broadcast_to(jnp.sum(sq.T, axis=0, keepdims=True), (8, T))
    for j in range(1, NH):
        power_copy(lax.rem(hd + j, NH), hd).start()

    def lower(x, y, z):
        return jnp.concatenate([cols(x, jnp.zeros_like(x)), cols(y, z)], axis=0)

    def stage_b(g, _):
        hs = [g * GB + i for i in range(GB)]
        fs = features([head_cols(q, h) for h in hs], [mq[h] for h in hs])
        gs = [khl[h] for h in hs]
        ss_ = [
            dot_t(f, cols(g[:, :DH], g[:, :DH])) + dot_t(f[:, :DH], g[:, DH:])
            for f, g in zip(fs, gs)
        ]
        for h, f, s in zip(hs, fs, ss_):
            x = jnp.where(tri, s[:DH, :DH], 0.0)
            y = s[DH:, :DH]
            z = jnp.where(tri, s[DH:, DH:], 0.0)
            (xh, xl), (yh, yl), (zh, zl) = split(x), split(y), split(z)
            ni[h] = dot(lower(xh, yh, zh), v[...]) + dot(lower(xl, yl, zl), v[...])
            dp[h, :DH] = x
            dp[h, DH:] = y + z
            qhl[h] = f
        return 0

    lax.fori_loop(0, NS // GB, stage_b, 0)

    def scan(phase, g, source, send, back, reverse):
        def step(j, total):
            s = NS - 1 - j if reverse else j

            @pl.when(s != me)
            def _():
                arrived(phase, g, source, s)

            send[g, s] = total
            return total + source[g, s]

        lax.fori_loop(0, NS, step, jnp.zeros((ROWS, DH), F32))
        send_all(phase + 1, g, send, back)
        back[g, me] = send[g, me]

    for g in range(NG):
        scan(0, g, a_recv, c_send, c_recv, False)

    power = p_send[...]
    for j in range(1, NH):
        power_copy(lax.rem(hd + j, NH), lax.rem(hd + j, NH)).wait_recv()
        power = power + p_recv[lax.rem(hd + j, NH)]
    power = power / (HEADS * DH) + 1e-05
    rp[...] = jnp.broadcast_to((1.0 / power).T[:, :1], (T, DH))

    def stage_d(g, cs, own):
        hs = [g * PG + c for c in cs]
        dsts = owners(cs, own)
        for o in dsts:
            arrived(1, g, c_recv, o)
        fs = [qhl[h] for h in hs]
        ws = []
        for c in cs:
            sh, sl = split(states(c_recv, g, c))
            ws.append(jnp.concatenate([cols(sh, sh), cols(sl, sl)], axis=0))
        numers = [ni[h] + fold(dot_t(f, w)) for h, f, w in zip(hs, fs, ws)]
        qfs = [join(f) for f in fs]
        dens = [
            jnp.sum(dp[h] + qf * totals(c_recv, g, c), axis=1, keepdims=True)
            for h, qf, c in zip(hs, qfs, cs)
        ]
        rdens = [1.0 / den for den in dens]
        students = [numer * rden for numer, rden in zip(numers, rdens)]
        gns = [
            (student - head_cols(t, h).astype(F32)) * rp[...] * rden
            for h, student, rden in zip(hs, students, rdens)
        ]
        gds = [-jnp.sum(gn * st, axis=1, keepdims=True) for gn, st in zip(gns, students)]
        ts = [split(gn.T) for gn in gns]
        outs = [fold(dot(th, f) + dot(tl, f)) for (th, tl), f in zip(ts, fs)]
        for c, h, qf, gn, gd, out in zip(cs, hs, qfs, gns, gds, outs):
            total = jnp.broadcast_to(jnp.sum(qf * gd, axis=0, keepdims=True), (8, DH))
            d_send[g, 2 * c, :HALF] = out[:HALF]
            d_send[g, 2 * c + 1, :HALF] = out[HALF:]
            d_send[g, 2 * c, HALF:] = total
            d_send[g, 2 * c + 1, HALF:] = total
            ghl[h] = cols(*split(gn))
            gd_s[h] = jnp.broadcast_to(gd, (T, DH))
        for o in dsts:
            seq_copy(2, g, d_send, d_recv, o).start()

    def rotated(stage, g, size):
        def heads(j0):
            return [lax.rem(mine - j0 - i + PG, PG) for i in range(size)][::-1]

        def step(j, _):
            stage(g, heads(j * size), False)
            return 0

        stage(g, heads(0), True)
        lax.fori_loop(1, PG // size, step, 0)

    def map_grads(xts, feats, grads):
        rs_ = [f * g for f, g in zip(feats, grads)]
        rs_ = [r - f * seg_sum(r) for r, f in zip(rs_, feats)]
        ys = [fold(dot(xt, cols(*split(r)))) for xt, r in zip(xts, rs_)]
        return [y - pltpu.roll(y, FH, 1) for y in ys]

    def stage_e(group, p):
        cs = [p * GE + i for i in range(GE)]
        hs = [group * PG + c for c in cs]
        gs = [ghl[h] for h in hs]
        bs = [dot_t(g, vv[...]) for g in gs]
        lows = []
        for h, b in zip(hs, bs):
            gd = gd_s[h]
            x = jnp.where(tri, b[:DH, :DH] + gd[:DH], 0.0)
            y = b[DH:, :DH] + gd[DH:]
            z = jnp.where(tri, b[DH:, DH:] + gd[DH:], 0.0)
            lows.append((split(x), split(y), split(z)))
        grads = []
        for c, h, g, (x, y, z) in zip(cs, hs, gs, lows):
            s = cols(*split(states(c_recv, group, c)))
            kf = khl[h]
            o = dot(g, jnp.concatenate([s, s], axis=0))
            o = o + dot(lower(x[0], y[0], z[0]), kf) + dot(lower(x[1], y[1], z[1]), kf)
            grads.append(fold(o) + gd_s[h] * totals(c_recv, group, c))
        fs = [qhl[h] for h in hs]
        outs = map_grads([head_cols(q, h).T for h in hs], [join(f) for f in fs], grads)
        for h, f, (x, y, z) in zip(hs, fs, lows):
            o = [
                dot(
                    jnp.concatenate(
                        [cols(x[i].T, y[i].T), cols(jnp.zeros_like(x[i]), z[i].T)], axis=0
                    ),
                    f,
                )
                for i in range(2)
            ]
            ni[h] = fold(o[0] + o[1])
        for i in range(0, GE, 2):
            both = jnp.where(even, outs[i], -outs[i + 1])
            gq_send[group, :, p * (GE // 2) + i // 2] = both.reshape(NS, 8, DH)

    for g in range(NG):
        rotated(stage_d, g, GD)
        d_recv[g, me] = d_send[g, me]

        def step_e(p, _, g=g):
            stage_e(g, p)
            return 0

        lax.fori_loop(0, PG // GE, step_e, 0)
        gq_recv[g, me] = gq_send[g, me]

    for g in range(NG):
        scan(2, g, d_recv, f_send, f_recv, True)
    for g in range(NG):
        send_all(4, g, gq_send, gq_recv)

    def stage_g(g, cs, own):
        hs = [g * PG + c for c in cs]
        for o in owners(cs, own):
            arrived(3, g, f_recv, o)
        ss_ = [cols(*split(states(f_recv, g, c))) for c in cs]
        grads = [
            ni[h] + fold(dot(v[...], s)) + totals(f_recv, g, c)
            for c, h, s in zip(cs, hs, ss_)
        ]
        outs = map_grads([k[...].T] * GG, [join(khl[h]) for h in hs], grads)
        for c, out in zip(cs, outs):
            odd = lax.rem(c, 2)
            sign = (1 - 2 * odd).astype(F32)
            own_half = jnp.where(even == (odd == 0), out * sign, 0.0)
            gk_sum[g, c // 2] += own_half

    gk_sum[...] = jnp.zeros_like(gk_sum)
    for g in range(NG):
        rotated(stage_g, g, GG)
        for p in range(PG // 2):
            gk_send[g, :, p] = gk_sum[g, p].reshape(NS, 8, DH)
        gk_recv[g, me] = gk_send[g, me]
        send_all(5, g, gk_send, gk_recv)

    def collect(phase, g, buf, out):
        def step(s, total):
            @pl.when(s != me)
            def _():
                arrived(phase, g, buf, s)

            return total + buf[g, s]

        total = lax.fori_loop(0, NS, step, jnp.zeros((PG // 2, 8, DH), F32))
        for p in range(PG // 2):
            out[g * PG + 2 * p] = total[p, :, :FH]
            out[g * PG + 2 * p + 1] = total[p, :, FH:]

    for g in range(NG):
        collect(4, g, gq_recv, oq)
    for g in range(NG):
        collect(5, g, gk_recv, ok)

    for phase, buf, dst_buf in (
        (0, a_send, a_recv),
        (1, c_send, c_recv),
        (2, d_send, d_recv),
        (3, f_send, f_recv),
        (4, gq_send, gq_recv),
        (5, gk_send, gk_recv),
    ):
        def drain(j, _, phase=phase, buf=buf, dst_buf=dst_buf):
            for g in range(NG):
                seq_copy(phase, g, buf, dst_buf, lax.rem(me + j, NS)).wait_send()
            return 0

        lax.fori_loop(1, NS, drain, 0)
    for j in range(1, NH):
        power_copy(lax.rem(hd + j, NH), hd).wait_send()


def on_device(queries, keys, values, teacher, map_q, map_k):
    state = pltpu.VMEM((NG, NS, ROWS, DH), F32)
    share = pltpu.VMEM((NG, NS, PG // 2, 8, DH), F32)
    pair = pltpu.VMEM((NS, T, 2 * DH), BF16)
    whole = pltpu.VMEM((NS, T, DH), F32)
    vmem = pl.BlockSpec(memory_space=pltpu.VMEM)
    out = jax.ShapeDtypeStruct((NS, 8, FH), F32)
    return pl.pallas_call(
        kernel,
        out_shape=(out, out),
        in_specs=[vmem] * 6,
        out_specs=(vmem, vmem),
        scratch_shapes=[
            pair, pair, pair,
            whole, whole, whole,
            pltpu.VMEM((T, DH), F32),
            pltpu.VMEM((DH + 16, T), BF16),
            pltpu.VMEM((T, 2 * DH), BF16),
            pltpu.VMEM((2 * DH, DH), BF16),
            pltpu.VMEM((8, T), F32),
            pltpu.VMEM((NH, 8, T), F32),
            state, state, state, state, state, state, state, state,
            share, share, share, share,
            pltpu.VMEM((NG, PG // 2, DH, DH), F32),
            pltpu.SemaphoreType.DMA((6, NG, NS)),
            pltpu.SemaphoreType.DMA((6, NG, NS)),
            pltpu.SemaphoreType.DMA((NH,)),
            pltpu.SemaphoreType.DMA((NH,)),
        ],
        compiler_params=pltpu.CompilerParams(
            collective_id=0, has_side_effects=True, vmem_limit_bytes=56 * 2**20
        ),
    )(queries, keys, values, teacher, map_q.swapaxes(1, 2), map_k.swapaxes(1, 2))


def solution(mesh):
    placed = (
        P("seq", "head"),
        P("seq", "head"),
        P("seq", "head"),
        P("seq", "head"),
        P("head", None, None),
        P("head", None, None),
    )
    return jax.shard_map(
        on_device,
        mesh=mesh,
        in_specs=placed,
        out_specs=(P("head", "seq", None), P("head", "seq", None)),
        check_vma=False,
    )
```

```python
import jax
import jax.numpy as jnp
from jax import lax
from jax.experimental import pallas as pl
from jax.experimental.pallas import tpu as pltpu
from jax.sharding import PartitionSpec as P

HEADS = 128
DH = 128
FH = 64
T = 256
NS = 16
NH = 8
NG = 2
PG = NS // NG
NO = NS // PG
PART = DH // NO
ROWS = PART + 8
SENT = PART + 1
GA, GB, GD, GE, GG = 4, 4, 2, 4, 2
MESH = pl.DeviceIdType.MESH
F32 = jnp.float32
BF16 = jnp.bfloat16


def split(x):
    high = x.astype(BF16)
    return high, (x - high.astype(F32)).astype(BF16)


def cols(x, y):
    return jnp.concatenate([x, y], axis=1)


def dot(a, b):
    return jnp.dot(a, b, preferred_element_type=F32)


def dot_t(a, b):
    return lax.dot_general(a, b, (((1,), (1,)), ((), ())), preferred_element_type=F32)


def join(x):
    return x[:, :DH].astype(F32) + x[:, DH:].astype(F32)


def fold(x):
    return x[:, :128] + x[:, 128:]


def kernel(
    q_in, k, v, t_in, mq_in, mk, oq, ok,
    q, t, mq, in_sem,
    khl, qhl, ghl, ni, dp, gd_s, rp, vta, vv, bb,
    p_send, p_recv, a_send, a_recv, c_send, c_recv, d_send, d_recv, f_send, f_recv,
    gq_send, gq_recv, gk_send, gk_recv, gk_sum,
    ss, rs, pss, prs,
):
    me = lax.axis_index("seq")
    hd = lax.axis_index("head")
    mine = me // NO
    siblings = [mine * NO + lax.rem(me + i, NO) for i in range(1, NO)]

    loads = [
        pltpu.make_async_copy(src, dst, in_sem.at[i])
        for i, (src, dst) in enumerate(((t_in, t), (q_in, q), (mq_in, mq)))
    ]
    for load in loads:
        load.start()

    barrier = pltpu.get_barrier_semaphore()
    for j in range(1, NS):
        pl.semaphore_signal(
            barrier, inc=1, device_id={"seq": lax.rem(me + j, NS)}, device_id_type=MESH
        )
    for j in range(1, NH):
        pl.semaphore_signal(
            barrier, inc=1, device_id={"head": lax.rem(hd + j, NH)}, device_id_type=MESH
        )

    def sent(buf, g, slot):
        if buf.shape[2] == ROWS:
            return buf.at[g, slot, pl.ds(0, SENT)]
        return buf.at[g, slot]

    def seq_copy(phase, g, buf, dst_buf, dst):
        return pltpu.make_async_remote_copy(
            src_ref=sent(buf, g, dst),
            dst_ref=sent(dst_buf, g, me),
            send_sem=ss.at[phase, g, dst],
            recv_sem=rs.at[phase, g, me],
            device_id={"seq": dst},
            device_id_type=MESH,
        )

    def arrived(phase, g, buf, slot):
        pltpu.make_async_remote_copy(
            src_ref=sent(buf, g, slot),
            dst_ref=sent(buf, g, slot),
            send_sem=ss.at[phase, g, slot],
            recv_sem=rs.at[phase, g, slot],
            device_id={"seq": slot},
            device_id_type=MESH,
        ).wait_recv()

    def send_all(phase, g, buf, dst_buf):
        def step(j, _):
            seq_copy(phase, g, buf, dst_buf, lax.rem(me + j, NS)).start()
            return 0

        lax.fori_loop(1, NS, step, 0)

    def owners(cs, own):
        return [NO * c + i for c in (cs[:-1] if own else cs) for i in range(NO)] + (
            siblings if own else []
        )

    def states(buf, g, c):
        return jnp.concatenate([buf[g, NO * c + i, :PART] for i in range(NO)], axis=0)

    def totals(buf, g, c):
        return buf[g, NO * c, PART:SENT]

    def put_state(buf, g, c, state, total):
        for i in range(NO):
            buf[g, NO * c + i, :PART] = state[i * PART : (i + 1) * PART]
            buf[g, NO * c + i, PART:] = total

    def power_copy(dst, slot):
        return pltpu.make_async_remote_copy(
            src_ref=p_send,
            dst_ref=p_recv.at[slot],
            send_sem=pss.at[dst],
            recv_sem=prs.at[slot],
            device_id={"head": dst},
            device_id_type=MESH,
        )

    def head_cols(ref, h):
        return ref[:, pl.ds(pl.multiple_of(h * DH, DH), DH)]

    even = lax.broadcasted_iota(jnp.int32, (DH, DH), 1) < FH

    row = lax.broadcasted_iota(jnp.int32, (2 * DH, DH), 0)
    col = lax.broadcasted_iota(jnp.int32, (2 * DH, DH), 1)
    bb[...] = jnp.where(lax.rem(row, DH) // FH == col // FH, 1.0, 0.0).astype(BF16)
    vta[:DH] = v[...].T
    vta[DH:] = jnp.ones((16, T), BF16)
    vv[...] = cols(v[...], v[...])

    tri = lax.broadcasted_iota(jnp.int32, (DH, DH), 0) >= lax.broadcasted_iota(
        jnp.int32, (DH, DH), 1
    )

    def seg_sum(x):
        return dot(cols(*split(x)), bb[...])

    def features(xs, ms):
        es = [jnp.exp(dot_t(x, jnp.concatenate([m, -m], axis=0))) for x, m in zip(xs, ms)]
        sums = [seg_sum(e) for e in es]
        return [cols(*split(e * (1.0 / z))) for e, z in zip(es, sums)]

    def stage_a(g, j0, own):
        cs = [lax.rem(mine + 1 + j0 + i, PG) for i in range(GA)]
        hs = [g * PG + c for c in cs]
        fs = features([k[...]] * GA, [mk[h] for h in hs])
        ps = [fold(dot(vta[...], f)) for f in fs]
        for c, h, f, p in zip(cs, hs, fs, ps):
            khl[h] = f
            put_state(a_send, g, c, p[:DH], p[DH : DH + 8])
        return owners(cs, own)

    for g in range(NG):
        for j0 in range(0, PG, GA):
            dsts = stage_a(g, j0, j0 + GA == PG)
            if g == 0 and j0 == 0:
                pl.semaphore_wait(barrier, NS + NH - 2)
            for dst in dsts:
                seq_copy(0, g, a_send, a_recv, dst).start()
        a_recv[g, me] = a_send[g, me]

    for load in loads:
        load.wait()

    def squares(j, total):
        x = head_cols(t, j).astype(F32)
        return total + x * x

    sq = lax.fori_loop(0, NS, squares, jnp.zeros((T, DH), F32))
    p_send[...] = jnp.broadcast_to(jnp.sum(sq.T, axis=0, keepdims=True), (8, T))
    for j in range(1, NH):
        power_copy(lax.rem(hd + j, NH), hd).start()

    def lower(x, y, z):
        return jnp.concatenate([cols(x, jnp.zeros_like(x)), cols(y, z)], axis=0)

    def stage_b(g, _):
        hs = [g * GB + i for i in range(GB)]
        fs = features([head_cols(q, h) for h in hs], [mq[h] for h in hs])
        gs = [khl[h] for h in hs]
        ss_ = [
            dot_t(f, cols(g[:, :DH], g[:, :DH])) + dot_t(f[:, :DH], g[:, DH:])
            for f, g in zip(fs, gs)
        ]
        for h, f, s in zip(hs, fs, ss_):
            x = jnp.where(tri, s[:DH, :DH], 0.0)
            y = s[DH:, :DH]
            z = jnp.where(tri, s[DH:, DH:], 0.0)
            (xh, xl), (yh, yl), (zh, zl) = split(x), split(y), split(z)
            ni[h] = dot(lower(xh, yh, zh), v[...]) + dot(lower(xl, yl, zl), v[...])
            dp[h, :DH] = x
            dp[h, DH:] = y + z
            qhl[h] = f
        return 0

    lax.fori_loop(0, NS // GB, stage_b, 0)

    def scan(phase, g, source, send, back, reverse):
        def step(j, total):
            s = NS - 1 - j if reverse else j

            @pl.when(s != me)
            def _():
                arrived(phase, g, source, s)

            send[g, s] = total
            return total + source[g, s]

        lax.fori_loop(0, NS, step, jnp.zeros((ROWS, DH), F32))
        send_all(phase + 1, g, send, back)
        back[g, me] = send[g, me]

    for g in range(NG):
        scan(0, g, a_recv, c_send, c_recv, False)

    power = p_send[...]
    for j in range(1, NH):
        power_copy(lax.rem(hd + j, NH), lax.rem(hd + j, NH)).wait_recv()
        power = power + p_recv[lax.rem(hd + j, NH)]
    power = power / (HEADS * DH) + 1e-05
    rp[...] = jnp.broadcast_to((1.0 / power).T[:, :1], (T, DH))

    def stage_d(g, cs, own):
        hs = [g * PG + c for c in cs]
        dsts = owners(cs, own)
        for o in dsts:
            arrived(1, g, c_recv, o)
        fs = [qhl[h] for h in hs]
        ws = []
        for c in cs:
            sh, sl = split(states(c_recv, g, c))
            ws.append(jnp.concatenate([cols(sh, sh), cols(sl, sl)], axis=0))
        numers = [ni[h] + fold(dot_t(f, w)) for h, f, w in zip(hs, fs, ws)]
        qfs = [join(f) for f in fs]
        dens = [
            jnp.sum(dp[h] + qf * totals(c_recv, g, c), axis=1, keepdims=True)
            for h, qf, c in zip(hs, qfs, cs)
        ]
        rdens = [1.0 / den for den in dens]
        students = [numer * rden for numer, rden in zip(numers, rdens)]
        gns = [
            (student - head_cols(t, h).astype(F32)) * rp[...] * rden
            for h, student, rden in zip(hs, students, rdens)
        ]
        gds = [-jnp.sum(gn * st, axis=1, keepdims=True) for gn, st in zip(gns, students)]
        ts = [split(gn.T) for gn in gns]
        outs = [fold(dot(th, f) + dot(tl, f)) for (th, tl), f in zip(ts, fs)]
        for c, h, qf, gn, gd, out in zip(cs, hs, qfs, gns, gds, outs):
            total = jnp.broadcast_to(jnp.sum(qf * gd, axis=0, keepdims=True), (8, DH))
            put_state(d_send, g, c, out, total)
            ghl[h] = cols(*split(gn))
            gd_s[h] = jnp.broadcast_to(gd, (T, DH))
        for o in dsts:
            seq_copy(2, g, d_send, d_recv, o).start()

    def rotated(stage, g, size):
        def heads(j0):
            return [lax.rem(mine - j0 - i + PG, PG) for i in range(size)][::-1]

        def step(j, _):
            stage(g, heads(j * size), False)
            return 0

        stage(g, heads(0), True)
        lax.fori_loop(1, PG // size, step, 0)

    def map_grads(xts, feats, grads):
        rs_ = [f * g for f, g in zip(feats, grads)]
        rs_ = [r - f * seg_sum(r) for r, f in zip(rs_, feats)]
        ys = [fold(dot(xt, cols(*split(r)))) for xt, r in zip(xts, rs_)]
        return [y - pltpu.roll(y, FH, 1) for y in ys]

    def stage_e(group, p):
        cs = [p * GE + i for i in range(GE)]
        hs = [group * PG + c for c in cs]
        gs = [ghl[h] for h in hs]
        bs = [dot_t(g, vv[...]) for g in gs]
        lows = []
        for h, b in zip(hs, bs):
            gd = gd_s[h]
            x = jnp.where(tri, b[:DH, :DH] + gd[:DH], 0.0)
            y = b[DH:, :DH] + gd[DH:]
            z = jnp.where(tri, b[DH:, DH:] + gd[DH:], 0.0)
            lows.append((split(x), split(y), split(z)))
        grads = []
        for c, h, g, (x, y, z) in zip(cs, hs, gs, lows):
            s = cols(*split(states(c_recv, group, c)))
            kf = khl[h]
            o = dot(g, jnp.concatenate([s, s], axis=0))
            o = o + dot(lower(x[0], y[0], z[0]), kf) + dot(lower(x[1], y[1], z[1]), kf)
            grads.append(fold(o) + gd_s[h] * totals(c_recv, group, c))
        fs = [qhl[h] for h in hs]
        outs = map_grads([head_cols(q, h).T for h in hs], [join(f) for f in fs], grads)
        for h, f, (x, y, z) in zip(hs, fs, lows):
            o = [
                dot(
                    jnp.concatenate(
                        [cols(x[i].T, y[i].T), cols(jnp.zeros_like(x[i]), z[i].T)], axis=0
                    ),
                    f,
                )
                for i in range(2)
            ]
            ni[h] = fold(o[0] + o[1])
        for i in range(0, GE, 2):
            both = jnp.where(even, outs[i], -outs[i + 1])
            gq_send[group, :, p * (GE // 2) + i // 2] = both.reshape(NS, 8, DH)

    def run_d(g):
        rotated(stage_d, g, GD)
        d_recv[g, me] = d_send[g, me]

    def run_e(g):
        def step_e(p, _):
            stage_e(g, p)
            return 0

        lax.fori_loop(0, PG // GE, step_e, 0)
        gq_recv[g, me] = gq_send[g, me]

    def run_f(g):
        scan(2, g, d_recv, f_send, f_recv, True)

    def run_q(g):
        send_all(4, g, gq_send, gq_recv)

    run_d(0)
    run_d(1)
    run_e(0)
    run_f(0)
    run_e(1)
    run_f(1)
    run_q(0)
    run_q(1)
    def stage_g(g, cs, own):
        hs = [g * PG + c for c in cs]
        for o in owners(cs, own):
            arrived(3, g, f_recv, o)
        ss_ = [cols(*split(states(f_recv, g, c))) for c in cs]
        grads = [
            ni[h] + fold(dot(v[...], s)) + totals(f_recv, g, c)
            for c, h, s in zip(cs, hs, ss_)
        ]
        outs = map_grads([k[...].T] * GG, [join(khl[h]) for h in hs], grads)
        for c, out in zip(cs, outs):
            odd = lax.rem(c, 2)
            sign = (1 - 2 * odd).astype(F32)
            own_half = jnp.where(even == (odd == 0), out * sign, 0.0)
            gk_sum[g, c // 2] += own_half

    gk_sum[...] = jnp.zeros_like(gk_sum)
    for g in range(NG):
        rotated(stage_g, g, GG)
        for p in range(PG // 2):
            gk_send[g, :, p] = gk_sum[g, p].reshape(NS, 8, DH)
        gk_recv[g, me] = gk_send[g, me]
        send_all(5, g, gk_send, gk_recv)

    def collect(phase, g, buf, out):
        def step(s, total):
            @pl.when(s != me)
            def _():
                arrived(phase, g, buf, s)

            return total + buf[g, s]

        total = lax.fori_loop(0, NS, step, jnp.zeros((PG // 2, 8, DH), F32))
        out[pl.ds(g * (PG // 2), PG // 2)] = total

    for g in range(NG):
        collect(4, g, gq_recv, oq)
    for g in range(NG):
        collect(5, g, gk_recv, ok)

    for phase, buf, dst_buf in (
        (0, a_send, a_recv),
        (1, c_send, c_recv),
        (2, d_send, d_recv),
        (3, f_send, f_recv),
        (4, gq_send, gq_recv),
        (5, gk_send, gk_recv),
    ):
        def drain(j, _, phase=phase, buf=buf, dst_buf=dst_buf):
            for g in range(NG):
                seq_copy(phase, g, buf, dst_buf, lax.rem(me + j, NS)).wait_send()
            return 0

        lax.fori_loop(1, NS, drain, 0)
    for j in range(1, NH):
        power_copy(lax.rem(hd + j, NH), hd).wait_send()


def unpack(pq, pk, oq, ok):
    for packed, out in ((pq, oq), (pk, ok)):
        for p in range(NS // 2):
            x = packed[p]
            out[2 * p] = x[:, :FH]
            out[2 * p + 1] = x[:, FH:]


def on_device(queries, keys, values, teacher, map_q, map_k):
    state = pltpu.VMEM((NG, NS, ROWS, DH), F32)
    share = pltpu.VMEM((NG, NS, PG // 2, 8, DH), F32)
    pair = pltpu.VMEM((NS, T, 2 * DH), BF16)
    whole = pltpu.VMEM((NS, T, DH), F32)
    vmem = pl.BlockSpec(memory_space=pltpu.VMEM)
    hbm = pl.BlockSpec(memory_space=pl.ANY)
    out = jax.ShapeDtypeStruct((NS // 2, 8, DH), F32)
    packed = pl.pallas_call(
        kernel,
        out_shape=(out, out),
        in_specs=[hbm, vmem, vmem, hbm, hbm, vmem],
        out_specs=(vmem, vmem),
        scratch_shapes=[
            pltpu.VMEM((T, NS * DH), BF16),
            pltpu.VMEM((T, NS * DH), BF16),
            pltpu.VMEM((NS, FH, DH), BF16),
            pltpu.SemaphoreType.DMA((3,)),
            pair, pair, pair,
            whole, whole, whole,
            pltpu.VMEM((T, DH), F32),
            pltpu.VMEM((DH + 16, T), BF16),
            pltpu.VMEM((T, 2 * DH), BF16),
            pltpu.VMEM((2 * DH, DH), BF16),
            pltpu.VMEM((8, T), F32),
            pltpu.VMEM((NH, 8, T), F32),
            state, state, state, state, state, state, state, state,
            share, share, share, share,
            pltpu.VMEM((NG, PG // 2, DH, DH), F32),
            pltpu.SemaphoreType.DMA((6, NG, NS)),
            pltpu.SemaphoreType.DMA((6, NG, NS)),
            pltpu.SemaphoreType.DMA((NH,)),
            pltpu.SemaphoreType.DMA((NH,)),
        ],
        compiler_params=pltpu.CompilerParams(
            collective_id=0, has_side_effects=True, vmem_limit_bytes=56 * 2**20
        ),
    )(queries, keys, values, teacher, map_q.swapaxes(1, 2), map_k.swapaxes(1, 2))

    final = jax.ShapeDtypeStruct((NS, 8, FH), F32)
    return pl.pallas_call(unpack, out_shape=(final, final))(*packed)


def solution(mesh):
    placed = (
        P("seq", "head"),
        P("seq", "head"),
        P("seq", "head"),
        P("seq", "head"),
        P("head", None, None),
        P("head", None, None),
    )
    return jax.shard_map(
        on_device,
        mesh=mesh,
        in_specs=placed,
        out_specs=(P("head", "seq", None), P("head", "seq", None)),
        check_vma=False,
    )
```

```python
import jax
import jax.numpy as jnp
from jax import lax
from jax.experimental import pallas as pl
from jax.experimental.pallas import tpu as pltpu
from jax.sharding import PartitionSpec as P

HEADS = 128
DH = 128
FH = 64
T = 256
NS = 16
NH = 8
NG = 2
PG = NS // NG
NO = NS // PG
PART = DH // NO
ROWS = PART + 8
SENT = PART + 1
GA, GB, GD, GE, GG = 4, 4, 2, 4, 4
MESH = pl.DeviceIdType.MESH
F32 = jnp.float32
BF16 = jnp.bfloat16


def split(x):
    high = x.astype(BF16)
    return high, (x - high.astype(F32)).astype(BF16)


def cols(x, y):
    return jnp.concatenate([x, y], axis=1)


def dot(a, b):
    return jnp.dot(a, b, preferred_element_type=F32)


def dot_t(a, b):
    return lax.dot_general(a, b, (((1,), (1,)), ((), ())), preferred_element_type=F32)


def join(x):
    return x[:, :DH].astype(F32) + x[:, DH:].astype(F32)


def fold(x):
    return x[:, :128] + x[:, 128:]


def kernel(
    q_in, k_in, v_in, t_in, mq_in, mk_in, oq, ok,
    q, t, mq, k, v, mk, in_sem,
    khl, qhl, ghl, ni, dp, gd_s, rp, vta, vv, bb,
    p_send, p_recv, a_send, a_recv, c_send, c_recv, d_send, d_recv, f_send, f_recv,
    gq_send, gq_recv, gk_send, gk_recv, gk_sum,
    ss, rs, pss, prs,
):
    me = lax.axis_index("seq")
    hd = lax.axis_index("head")
    mine = me // NO
    siblings = [mine * NO + lax.rem(me + i, NO) for i in range(1, NO)]

    loads = [
        pltpu.make_async_copy(src, dst, in_sem.at[i])
        for i, (src, dst) in enumerate(
            ((k_in, k), (mk_in, mk), (v_in, v), (t_in, t), (q_in, q), (mq_in, mq))
        )
    ]
    for load in loads:
        load.start()

    barrier = pltpu.get_barrier_semaphore()
    for j in range(1, NS):
        pl.semaphore_signal(
            barrier, inc=1, device_id={"seq": lax.rem(me + j, NS)}, device_id_type=MESH
        )
    for j in range(1, NH):
        pl.semaphore_signal(
            barrier, inc=1, device_id={"head": lax.rem(hd + j, NH)}, device_id_type=MESH
        )

    def sent(buf, g, slot):
        if buf.shape[2] == ROWS:
            return buf.at[g, slot, pl.ds(0, SENT)]
        return buf.at[g, slot]

    def seq_copy(phase, g, buf, dst_buf, dst):
        return pltpu.make_async_remote_copy(
            src_ref=sent(buf, g, dst),
            dst_ref=sent(dst_buf, g, me),
            send_sem=ss.at[phase, g, dst],
            recv_sem=rs.at[phase, g, me],
            device_id={"seq": dst},
            device_id_type=MESH,
        )

    def arrived(phase, g, buf, slot):
        pltpu.make_async_remote_copy(
            src_ref=sent(buf, g, slot),
            dst_ref=sent(buf, g, slot),
            send_sem=ss.at[phase, g, slot],
            recv_sem=rs.at[phase, g, slot],
            device_id={"seq": slot},
            device_id_type=MESH,
        ).wait_recv()

    def send_all(phase, g, buf, dst_buf):
        if phase >= 4:
            hops = sorted(range(1, NS), key=lambda i: -min(i // 4, 4 - i // 4) - min(i % 4, 4 - i % 4))
            for i in hops:
                y, x = lax.rem(me // 4 + i // 4, 4), lax.rem(me + i, 4)
                seq_copy(phase, g, buf, dst_buf, 4 * y + x).start()
            return

        def step(j, _):
            seq_copy(phase, g, buf, dst_buf, lax.rem(me + j, NS)).start()
            return 0

        lax.fori_loop(1, NS, step, 0)

    def owners(cs, own):
        return [NO * c + i for c in (cs[:-1] if own else cs) for i in range(NO)] + (
            siblings if own else []
        )

    def states(buf, g, c):
        return jnp.concatenate([buf[g, NO * c + i, :PART] for i in range(NO)], axis=0)

    def totals(buf, g, c):
        return buf[g, NO * c, PART:SENT]

    def put_state(buf, g, c, state, total):
        for i in range(NO):
            buf[g, NO * c + i, :PART] = state[i * PART : (i + 1) * PART]
            buf[g, NO * c + i, PART:] = total

    def power_copy(dst, slot):
        return pltpu.make_async_remote_copy(
            src_ref=p_send,
            dst_ref=p_recv.at[slot],
            send_sem=pss.at[dst],
            recv_sem=prs.at[slot],
            device_id={"head": dst},
            device_id_type=MESH,
        )

    def head_cols(ref, h):
        return ref[:, pl.ds(pl.multiple_of(h * DH, DH), DH)]

    even = lax.broadcasted_iota(jnp.int32, (DH, DH), 1) < FH

    row = lax.broadcasted_iota(jnp.int32, (2 * DH, DH), 0)
    col = lax.broadcasted_iota(jnp.int32, (2 * DH, DH), 1)
    bb[...] = jnp.where(lax.rem(row, DH) // FH == col // FH, 1.0, 0.0).astype(BF16)
    for load in loads[:3]:
        load.wait()
    vta[:DH] = v[...].T
    vta[DH:] = jnp.ones((16, T), BF16)
    vv[...] = cols(v[...], v[...])

    tri = lax.broadcasted_iota(jnp.int32, (DH, DH), 0) >= lax.broadcasted_iota(
        jnp.int32, (DH, DH), 1
    )

    def seg_sum(x):
        return dot(cols(*split(x)), bb[...])

    def features(xs, ms):
        es = [jnp.exp(dot_t(x, jnp.concatenate([m, -m], axis=0))) for x, m in zip(xs, ms)]
        sums = [seg_sum(e) for e in es]
        return [cols(*split(e * (1.0 / z))) for e, z in zip(es, sums)]

    def stage_a(g, j0, own):
        cs = [lax.rem(mine + 1 + j0 + i, PG) for i in range(GA)]
        hs = [g * PG + c for c in cs]
        fs = features([k[...]] * GA, [mk[h] for h in hs])
        ps = [fold(dot(vta[...], f)) for f in fs]
        for c, h, f, p in zip(cs, hs, fs, ps):
            khl[h] = f
            put_state(a_send, g, c, p[:DH], p[DH : DH + 8])
        return owners(cs, own)

    for g in range(NG):
        for j0 in range(0, PG, GA):
            dsts = stage_a(g, j0, j0 + GA == PG)
            if g == 0 and j0 == 0:
                pl.semaphore_wait(barrier, NS + NH - 2)
            for dst in dsts:
                seq_copy(0, g, a_send, a_recv, dst).start()
        a_recv[g, me] = a_send[g, me]

    for load in loads[3:]:
        load.wait()

    def squares(j, total):
        x = head_cols(t, j).astype(F32)
        return total + x * x

    sq = lax.fori_loop(0, NS, squares, jnp.zeros((T, DH), F32))
    p_send[...] = jnp.broadcast_to(jnp.sum(sq.T, axis=0, keepdims=True), (8, T))
    for j in range(1, NH):
        power_copy(lax.rem(hd + j, NH), hd).start()

    def lower(x, y, z):
        return jnp.concatenate([cols(x, jnp.zeros_like(x)), cols(y, z)], axis=0)

    def stage_b(g, _):
        hs = [g * GB + i for i in range(GB)]
        fs = features([head_cols(q, h) for h in hs], [mq[h] for h in hs])
        gs = [khl[h] for h in hs]
        ss_ = [
            dot_t(f, cols(g[:, :DH], g[:, :DH])) + dot_t(f[:, :DH], g[:, DH:])
            for f, g in zip(fs, gs)
        ]
        for h, f, s in zip(hs, fs, ss_):
            x = jnp.where(tri, s[:DH, :DH], 0.0)
            y = s[DH:, :DH]
            z = jnp.where(tri, s[DH:, DH:], 0.0)
            (xh, xl), (yh, yl), (zh, zl) = split(x), split(y), split(z)
            ni[h] = dot(lower(xh, yh, zh), v[...]) + dot(lower(xl, yl, zl), v[...])
            dp[h, :DH] = x
            dp[h, DH:] = y + z
            qhl[h] = f
        return 0

    lax.fori_loop(0, NS // GB, stage_b, 0)

    def scan(phase, g, source, send, back, reverse):
        def step(j, total):
            s = NS - 1 - j if reverse else j

            @pl.when(s != me)
            def _():
                arrived(phase, g, source, s)

            send[g, s] = total
            return total + source[g, s]

        lax.fori_loop(0, NS, step, jnp.zeros((ROWS, DH), F32))
        send_all(phase + 1, g, send, back)
        back[g, me] = send[g, me]

    for g in range(NG):
        scan(0, g, a_recv, c_send, c_recv, False)

    power = p_send[...]
    for j in range(1, NH):
        power_copy(lax.rem(hd + j, NH), lax.rem(hd + j, NH)).wait_recv()
        power = power + p_recv[lax.rem(hd + j, NH)]
    power = power / (HEADS * DH) + 1e-05
    rp[...] = jnp.broadcast_to((1.0 / power).T[:, :1], (T, DH))

    def stage_d(g, cs, own):
        hs = [g * PG + c for c in cs]
        dsts = owners(cs, own)
        for o in dsts:
            arrived(1, g, c_recv, o)
        fs = [qhl[h] for h in hs]
        ws = []
        for c in cs:
            sh, sl = split(states(c_recv, g, c))
            ws.append(jnp.concatenate([cols(sh, sh), cols(sl, sl)], axis=0))
        numers = [ni[h] + fold(dot_t(f, w)) for h, f, w in zip(hs, fs, ws)]
        qfs = [join(f) for f in fs]
        dens = [
            jnp.sum(dp[h] + qf * totals(c_recv, g, c), axis=1, keepdims=True)
            for h, qf, c in zip(hs, qfs, cs)
        ]
        rdens = [1.0 / den for den in dens]
        students = [numer * rden for numer, rden in zip(numers, rdens)]
        gns = [
            (student - head_cols(t, h).astype(F32)) * rp[...] * rden
            for h, student, rden in zip(hs, students, rdens)
        ]
        gds = [-jnp.sum(gn * st, axis=1, keepdims=True) for gn, st in zip(gns, students)]
        ts = [split(gn.T) for gn in gns]
        outs = [fold(dot(th, f) + dot(tl, f)) for (th, tl), f in zip(ts, fs)]
        for c, h, qf, gn, gd, out in zip(cs, hs, qfs, gns, gds, outs):
            total = jnp.broadcast_to(jnp.sum(qf * gd, axis=0, keepdims=True), (8, DH))
            put_state(d_send, g, c, out, total)
            ghl[h] = cols(*split(gn))
            gd_s[h] = jnp.broadcast_to(gd, (T, DH))
        for o in dsts:
            seq_copy(2, g, d_send, d_recv, o).start()

    def rotated(stage, g, size):
        def heads(j0):
            return [lax.rem(mine - j0 - i + PG, PG) for i in range(size)][::-1]

        def step(j, _):
            stage(g, heads(j * size), False)
            return 0

        stage(g, heads(0), True)
        lax.fori_loop(1, PG // size, step, 0)

    def map_grads(xts, feats, grads):
        rs_ = [f * g for f, g in zip(feats, grads)]
        rs_ = [r - f * seg_sum(r) for r, f in zip(rs_, feats)]
        ys = [fold(dot(xt, cols(*split(r)))) for xt, r in zip(xts, rs_)]
        return [y - pltpu.roll(y, FH, 1) for y in ys]

    def stage_e(group, p):
        cs = [p * GE + i for i in range(GE)]
        hs = [group * PG + c for c in cs]
        gs = [ghl[h] for h in hs]
        bs = [dot_t(g, vv[...]) for g in gs]
        lows = []
        for h, b in zip(hs, bs):
            gd = gd_s[h]
            x = jnp.where(tri, b[:DH, :DH] + gd[:DH], 0.0)
            y = b[DH:, :DH] + gd[DH:]
            z = jnp.where(tri, b[DH:, DH:] + gd[DH:], 0.0)
            lows.append((split(x), split(y), split(z)))
        grads = []
        for c, h, g, (x, y, z) in zip(cs, hs, gs, lows):
            s = cols(*split(states(c_recv, group, c)))
            kf = khl[h]
            o = dot(g, jnp.concatenate([s, s], axis=0))
            o = o + dot(lower(x[0], y[0], z[0]), kf) + dot(lower(x[1], y[1], z[1]), kf)
            grads.append(fold(o) + gd_s[h] * totals(c_recv, group, c))
        fs = [qhl[h] for h in hs]
        outs = map_grads([head_cols(q, h).T for h in hs], [join(f) for f in fs], grads)
        for h, f, (x, y, z) in zip(hs, fs, lows):
            o = [
                dot(
                    jnp.concatenate(
                        [cols(x[i].T, y[i].T), cols(jnp.zeros_like(x[i]), z[i].T)], axis=0
                    ),
                    f,
                )
                for i in range(2)
            ]
            ni[h] = fold(o[0] + o[1])
        for i in range(0, GE, 2):
            both = jnp.where(even, outs[i], -outs[i + 1])
            gq_send[group, :, p * (GE // 2) + i // 2] = both.reshape(NS, 8, DH)

    def run_d(g):
        rotated(stage_d, g, GD)
        d_recv[g, me] = d_send[g, me]

    def run_e(g):
        def step_e(p, _):
            stage_e(g, p)
            return 0

        lax.fori_loop(0, PG // GE, step_e, 0)
        gq_recv[g, me] = gq_send[g, me]

    def run_f(g):
        scan(2, g, d_recv, f_send, f_recv, True)

    def run_q(g):
        send_all(4, g, gq_send, gq_recv)

    run_d(0)
    run_d(1)
    run_e(0)
    run_f(0)
    run_e(1)
    run_f(1)
    run_q(0)
    run_q(1)
    def stage_g(g, cs, own):
        hs = [g * PG + c for c in cs]
        for o in owners(cs, own):
            arrived(3, g, f_recv, o)
        ss_ = [cols(*split(states(f_recv, g, c))) for c in cs]
        grads = [
            ni[h] + fold(dot(v[...], s)) + totals(f_recv, g, c)
            for c, h, s in zip(cs, hs, ss_)
        ]
        outs = map_grads([k[...].T] * GG, [join(khl[h]) for h in hs], grads)
        for c, out in zip(cs, outs):
            odd = lax.rem(c, 2)
            sign = (1 - 2 * odd).astype(F32)
            own_half = jnp.where(even == (odd == 0), out * sign, 0.0)
            gk_sum[g, c // 2] += own_half

    gk_sum[...] = jnp.zeros_like(gk_sum)
    for g in range(NG):
        rotated(stage_g, g, GG)
        for p in range(PG // 2):
            gk_send[g, :, p] = gk_sum[g, p].reshape(NS, 8, DH)
        gk_recv[g, me] = gk_send[g, me]
        send_all(5, g, gk_send, gk_recv)

    def collect(phase, g, buf, out):
        def step(s, total):
            @pl.when(s != me)
            def _():
                arrived(phase, g, buf, s)

            return total + buf[g, s]

        total = lax.fori_loop(0, NS, step, jnp.zeros((PG // 2, 8, DH), F32))
        out[pl.ds(g * (PG // 2), PG // 2)] = total

    for g in range(NG):
        collect(4, g, gq_recv, oq)
    for g in range(NG):
        collect(5, g, gk_recv, ok)

    for phase, buf, dst_buf in (
        (0, a_send, a_recv),
        (1, c_send, c_recv),
        (2, d_send, d_recv),
        (3, f_send, f_recv),
        (4, gq_send, gq_recv),
        (5, gk_send, gk_recv),
    ):
        def drain(j, _, phase=phase, buf=buf, dst_buf=dst_buf):
            for g in range(NG):
                seq_copy(phase, g, buf, dst_buf, lax.rem(me + j, NS)).wait_send()
            return 0

        lax.fori_loop(1, NS, drain, 0)
    for j in range(1, NH):
        power_copy(lax.rem(hd + j, NH), hd).wait_send()


def unpack(pq, pk, oq, ok):
    for packed, out in ((pq, oq), (pk, ok)):
        for p in range(NS // 2):
            x = packed[p]
            out[2 * p] = x[:, :FH]
            out[2 * p + 1] = x[:, FH:]


def on_device(queries, keys, values, teacher, map_q, map_k):
    state = pltpu.VMEM((NG, NS, ROWS, DH), F32)
    share = pltpu.VMEM((NG, NS, PG // 2, 8, DH), F32)
    pair = pltpu.VMEM((NS, T, 2 * DH), BF16)
    whole = pltpu.VMEM((NS, T, DH), F32)
    vmem = pl.BlockSpec(memory_space=pltpu.VMEM)
    hbm = pl.BlockSpec(memory_space=pl.ANY)
    out = jax.ShapeDtypeStruct((NS // 2, 8, DH), F32)
    packed = pl.pallas_call(
        kernel,
        out_shape=(out, out),
        in_specs=[hbm] * 6,
        out_specs=(vmem, vmem),
        scratch_shapes=[
            pltpu.VMEM((T, NS * DH), BF16),
            pltpu.VMEM((T, NS * DH), BF16),
            pltpu.VMEM((NS, FH, DH), BF16),
            pltpu.VMEM((T, DH), BF16),
            pltpu.VMEM((T, DH), BF16),
            pltpu.VMEM((NS, FH, DH), BF16),
            pltpu.SemaphoreType.DMA((6,)),
            pair, pair, pair,
            whole, whole, whole,
            pltpu.VMEM((T, DH), F32),
            pltpu.VMEM((DH + 16, T), BF16),
            pltpu.VMEM((T, 2 * DH), BF16),
            pltpu.VMEM((2 * DH, DH), BF16),
            pltpu.VMEM((8, T), F32),
            pltpu.VMEM((NH, 8, T), F32),
            state, state, state, state, state, state, state, state,
            share, share, share, share,
            pltpu.VMEM((NG, PG // 2, DH, DH), F32),
            pltpu.SemaphoreType.DMA((6, NG, NS)),
            pltpu.SemaphoreType.DMA((6, NG, NS)),
            pltpu.SemaphoreType.DMA((NH,)),
            pltpu.SemaphoreType.DMA((NH,)),
        ],
        compiler_params=pltpu.CompilerParams(
            collective_id=0, has_side_effects=True, vmem_limit_bytes=56 * 2**20
        ),
    )(queries, keys, values, teacher, map_q.swapaxes(1, 2), map_k.swapaxes(1, 2))

    final = jax.ShapeDtypeStruct((NS, 8, FH), F32)
    return pl.pallas_call(unpack, out_shape=(final, final))(*packed)


def solution(mesh):
    placed = (
        P("seq", "head"),
        P("seq", "head"),
        P("seq", "head"),
        P("seq", "head"),
        P("head", None, None),
        P("head", None, None),
    )
    return jax.shard_map(
        on_device,
        mesh=mesh,
        in_specs=placed,
        out_specs=(P("head", "seq", None), P("head", "seq", None)),
        check_vma=False,
    )
```

```python
import jax
import jax.numpy as jnp
from jax import lax
from jax.experimental import pallas as pl
from jax.experimental.pallas import tpu as pltpu
from jax.sharding import PartitionSpec as P

HEADS = 128
DH = 128
FH = 64
T = 256
NS = 16
NH = 8
NG = 2
PG = NS // NG
NO = NS // PG
PART = DH // NO
ROWS = PART + 8
SENT = PART + 1
GA, GB, GD, GE, GG = 2, 4, 2, 4, 4
MESH = pl.DeviceIdType.MESH
F32 = jnp.float32
BF16 = jnp.bfloat16


def split(x):
    high = x.astype(BF16)
    return high, (x - high.astype(F32)).astype(BF16)


def cols(x, y):
    return jnp.concatenate([x, y], axis=1)


def dot(a, b):
    return jnp.dot(a, b, preferred_element_type=F32)


def dot_t(a, b):
    return lax.dot_general(a, b, (((1,), (1,)), ((), ())), preferred_element_type=F32)


def join(x):
    return x[:, :DH].astype(F32) + x[:, DH:].astype(F32)


def fold(x):
    return x[:, :128] + x[:, 128:]


def kernel(
    q_in, k_in, v_in, t_in, mq_in, mk_in, oq, ok,
    q, t, mq, k, v, mk, in_sem,
    khl, qhl, ghl, ni, dp, gd_s, rp, vta, vv, bb,
    p_send, p_recv, a_send, a_recv, c_send, c_recv, d_send, d_recv, f_send, f_recv,
    gq_send, gq_recv, gk_send, gk_recv, gk_sum,
    ss, rs, pss, prs,
):
    me = lax.axis_index("seq")
    hd = lax.axis_index("head")
    mine = me // NO
    siblings = [mine * NO + lax.rem(me + i, NO) for i in range(1, NO)]

    loads = [
        pltpu.make_async_copy(src, dst, in_sem.at[i])
        for i, (src, dst) in enumerate(
            ((k_in, k), (mk_in, mk), (v_in, v), (t_in, t), (q_in, q), (mq_in, mq))
        )
    ]
    for load in loads:
        load.start()

    barrier = pltpu.get_barrier_semaphore()
    for j in range(1, NS):
        pl.semaphore_signal(
            barrier, inc=1, device_id={"seq": lax.rem(me + j, NS)}, device_id_type=MESH
        )
    for j in range(1, NH):
        pl.semaphore_signal(
            barrier, inc=1, device_id={"head": lax.rem(hd + j, NH)}, device_id_type=MESH
        )

    def sent(buf, g, slot):
        if buf.shape[2] == ROWS:
            return buf.at[g, slot, pl.ds(0, SENT)]
        return buf.at[g, slot]

    def seq_copy(phase, g, buf, dst_buf, dst):
        return pltpu.make_async_remote_copy(
            src_ref=sent(buf, g, dst),
            dst_ref=sent(dst_buf, g, me),
            send_sem=ss.at[phase, g, dst],
            recv_sem=rs.at[phase, g, me],
            device_id={"seq": dst},
            device_id_type=MESH,
        )

    def arrived(phase, g, buf, slot):
        pltpu.make_async_remote_copy(
            src_ref=sent(buf, g, slot),
            dst_ref=sent(buf, g, slot),
            send_sem=ss.at[phase, g, slot],
            recv_sem=rs.at[phase, g, slot],
            device_id={"seq": slot},
            device_id_type=MESH,
        ).wait_recv()

    def send_all(phase, g, buf, dst_buf):
        if phase >= 4:
            hops = sorted(range(1, NS), key=lambda i: -min(i // 4, 4 - i // 4) - min(i % 4, 4 - i % 4))
            for i in hops:
                y, x = lax.rem(me // 4 + i // 4, 4), lax.rem(me + i, 4)
                seq_copy(phase, g, buf, dst_buf, 4 * y + x).start()
            return

        def step(j, _):
            seq_copy(phase, g, buf, dst_buf, lax.rem(me + j, NS)).start()
            return 0

        lax.fori_loop(1, NS, step, 0)

    def owners(cs, own):
        return [NO * c + i for c in (cs[:-1] if own else cs) for i in range(NO)] + (
            siblings if own else []
        )

    def states(buf, g, c):
        return jnp.concatenate([buf[g, NO * c + i, :PART] for i in range(NO)], axis=0)

    def totals(buf, g, c):
        return buf[g, NO * c, PART:SENT]

    def put_state(buf, g, c, state, total):
        for i in range(NO):
            buf[g, NO * c + i, :PART] = state[i * PART : (i + 1) * PART]
            buf[g, NO * c + i, PART:] = total

    def power_copy(dst, slot):
        return pltpu.make_async_remote_copy(
            src_ref=p_send,
            dst_ref=p_recv.at[slot],
            send_sem=pss.at[dst],
            recv_sem=prs.at[slot],
            device_id={"head": dst},
            device_id_type=MESH,
        )

    def head_cols(ref, h):
        return ref[:, pl.ds(pl.multiple_of(h * DH, DH), DH)]

    even = lax.broadcasted_iota(jnp.int32, (DH, DH), 1) < FH

    row = lax.broadcasted_iota(jnp.int32, (2 * DH, DH), 0)
    col = lax.broadcasted_iota(jnp.int32, (2 * DH, DH), 1)
    bb[...] = jnp.where(lax.rem(row, DH) // FH == col // FH, 1.0, 0.0).astype(BF16)
    for load in loads[:3]:
        load.wait()
    vta[:DH] = v[...].T
    vta[DH:] = jnp.ones((16, T), BF16)
    vv[...] = cols(v[...], v[...])

    tri = lax.broadcasted_iota(jnp.int32, (DH, DH), 0) >= lax.broadcasted_iota(
        jnp.int32, (DH, DH), 1
    )

    def seg_sum(x):
        return dot(cols(*split(x)), bb[...])

    def features(xs, ms):
        es = [jnp.exp(dot_t(x, jnp.concatenate([m, -m], axis=0))) for x, m in zip(xs, ms)]
        sums = [seg_sum(e) for e in es]
        return [cols(*split(e * (1.0 / z))) for e, z in zip(es, sums)]

    def stage_a(g, j0, own):
        cs = [lax.rem(mine + 1 + j0 + i, PG) for i in range(GA)]
        hs = [g * PG + c for c in cs]
        fs = features([k[...]] * GA, [mk[h] for h in hs])
        ps = [fold(dot(vta[...], f)) for f in fs]
        for c, h, f, p in zip(cs, hs, fs, ps):
            khl[h] = f
            put_state(a_send, g, c, p[:DH], p[DH : DH + 8])
        return owners(cs, own)

    for g in range(NG):
        for j0 in range(0, PG, GA):
            dsts = stage_a(g, j0, j0 + GA == PG)
            if g == 0 and j0 == 0:
                pl.semaphore_wait(barrier, NS + NH - 2)
            for dst in dsts:
                seq_copy(0, g, a_send, a_recv, dst).start()
        a_recv[g, me] = a_send[g, me]

    for load in loads[3:]:
        load.wait()

    def squares(j, total):
        x = head_cols(t, j).astype(F32)
        return total + x * x

    sq = lax.fori_loop(0, NS, squares, jnp.zeros((T, DH), F32))
    p_send[...] = jnp.broadcast_to(jnp.sum(sq.T, axis=0, keepdims=True), (8, T))
    for j in range(1, NH):
        power_copy(lax.rem(hd + j, NH), hd).start()

    def lower(x, y, z):
        return jnp.concatenate([cols(x, jnp.zeros_like(x)), cols(y, z)], axis=0)

    def stage_b(g, _):
        hs = [g * GB + i for i in range(GB)]
        fs = features([head_cols(q, h) for h in hs], [mq[h] for h in hs])
        gs = [khl[h] for h in hs]
        ss_ = [
            dot_t(f, cols(g[:, :DH], g[:, :DH])) + dot_t(f[:, :DH], g[:, DH:])
            for f, g in zip(fs, gs)
        ]
        for h, f, s in zip(hs, fs, ss_):
            x = jnp.where(tri, s[:DH, :DH], 0.0)
            y = s[DH:, :DH]
            z = jnp.where(tri, s[DH:, DH:], 0.0)
            (xh, xl), (yh, yl), (zh, zl) = split(x), split(y), split(z)
            ni[h] = dot(lower(xh, yh, zh), v[...]) + dot(lower(xl, yl, zl), v[...])
            dp[h, :DH] = x
            dp[h, DH:] = y + z
            qhl[h] = f
        return 0

    lax.fori_loop(0, NS // GB, stage_b, 0)

    def scan(phase, g, source, send, back, reverse):
        def step(j, total):
            s = NS - 1 - j if reverse else j

            @pl.when(s != me)
            def _():
                arrived(phase, g, source, s)

            send[g, s] = total
            return total + source[g, s]

        lax.fori_loop(0, NS, step, jnp.zeros((ROWS, DH), F32))
        send_all(phase + 1, g, send, back)
        back[g, me] = send[g, me]

    for g in range(NG):
        scan(0, g, a_recv, c_send, c_recv, False)

    power = p_send[...]
    for j in range(1, NH):
        power_copy(lax.rem(hd + j, NH), lax.rem(hd + j, NH)).wait_recv()
        power = power + p_recv[lax.rem(hd + j, NH)]
    power = power / (HEADS * DH) + 1e-05
    rp[...] = jnp.broadcast_to((1.0 / power).T[:, :1], (T, DH))

    def stage_d(g, cs, own):
        hs = [g * PG + c for c in cs]
        dsts = owners(cs, own)
        for o in dsts:
            arrived(1, g, c_recv, o)
        fs = [qhl[h] for h in hs]
        ws = []
        for c in cs:
            sh, sl = split(states(c_recv, g, c))
            ws.append(jnp.concatenate([cols(sh, sh), cols(sl, sl)], axis=0))
        numers = [ni[h] + fold(dot_t(f, w)) for h, f, w in zip(hs, fs, ws)]
        qfs = [join(f) for f in fs]
        dens = [
            jnp.sum(dp[h] + qf * totals(c_recv, g, c), axis=1, keepdims=True)
            for h, qf, c in zip(hs, qfs, cs)
        ]
        rdens = [1.0 / den for den in dens]
        students = [numer * rden for numer, rden in zip(numers, rdens)]
        gns = [
            (student - head_cols(t, h).astype(F32)) * rp[...] * rden
            for h, student, rden in zip(hs, students, rdens)
        ]
        gds = [-jnp.sum(gn * st, axis=1, keepdims=True) for gn, st in zip(gns, students)]
        ts = [split(gn.T) for gn in gns]
        outs = [fold(dot(th, f) + dot(tl, f)) for (th, tl), f in zip(ts, fs)]
        for c, h, qf, gn, gd, out in zip(cs, hs, qfs, gns, gds, outs):
            total = jnp.broadcast_to(jnp.sum(qf * gd, axis=0, keepdims=True), (8, DH))
            put_state(d_send, g, c, out, total)
            ghl[h] = cols(*split(gn))
            gd_s[h] = jnp.broadcast_to(gd, (T, DH))
        for o in dsts:
            seq_copy(2, g, d_send, d_recv, o).start()

    def rotated(stage, g, size):
        def heads(j0):
            return [lax.rem(mine - j0 - i + PG, PG) for i in range(size)][::-1]

        def step(j, _):
            stage(g, heads(j * size), False)
            return 0

        stage(g, heads(0), True)
        lax.fori_loop(1, PG // size, step, 0)

    def map_grads(xts, feats, grads):
        rs_ = [f * g for f, g in zip(feats, grads)]
        rs_ = [r - f * seg_sum(r) for r, f in zip(rs_, feats)]
        ys = [fold(dot(xt, cols(*split(r)))) for xt, r in zip(xts, rs_)]
        return [y - pltpu.roll(y, FH, 1) for y in ys]

    def stage_e(group, p):
        cs = [p * GE + i for i in range(GE)]
        hs = [group * PG + c for c in cs]
        gs = [ghl[h] for h in hs]
        bs = [dot_t(g, vv[...]) for g in gs]
        lows = []
        for h, b in zip(hs, bs):
            gd = gd_s[h]
            x = jnp.where(tri, b[:DH, :DH] + gd[:DH], 0.0)
            y = b[DH:, :DH] + gd[DH:]
            z = jnp.where(tri, b[DH:, DH:] + gd[DH:], 0.0)
            lows.append((split(x), split(y), split(z)))
        grads = []
        for c, h, g, (x, y, z) in zip(cs, hs, gs, lows):
            s = cols(*split(states(c_recv, group, c)))
            kf = khl[h]
            o = dot(g, jnp.concatenate([s, s], axis=0))
            o = o + dot(lower(x[0], y[0], z[0]), kf) + dot(lower(x[1], y[1], z[1]), kf)
            grads.append(fold(o) + gd_s[h] * totals(c_recv, group, c))
        fs = [qhl[h] for h in hs]
        outs = map_grads([head_cols(q, h).T for h in hs], [join(f) for f in fs], grads)
        for h, f, (x, y, z) in zip(hs, fs, lows):
            o = [
                dot(
                    jnp.concatenate(
                        [cols(x[i].T, y[i].T), cols(jnp.zeros_like(x[i]), z[i].T)], axis=0
                    ),
                    f,
                )
                for i in range(2)
            ]
            ni[h] = fold(o[0] + o[1])
        for i in range(0, GE, 2):
            both = jnp.where(even, outs[i], -outs[i + 1])
            gq_send[group, :, p * (GE // 2) + i // 2] = both.reshape(NS, 8, DH)

    def run_d(g):
        rotated(stage_d, g, GD)
        d_recv[g, me] = d_send[g, me]

    def run_e(g):
        def step_e(p, _):
            stage_e(g, p)
            return 0

        lax.fori_loop(0, PG // GE, step_e, 0)
        gq_recv[g, me] = gq_send[g, me]

    def run_f(g):
        scan(2, g, d_recv, f_send, f_recv, True)

    def run_q(g):
        send_all(4, g, gq_send, gq_recv)

    run_d(0)
    run_d(1)
    run_e(0)
    run_f(0)
    run_e(1)
    run_f(1)
    run_q(0)
    run_q(1)
    def stage_g(g, cs, own):
        hs = [g * PG + c for c in cs]
        for o in owners(cs, own):
            arrived(3, g, f_recv, o)
        ss_ = [cols(*split(states(f_recv, g, c))) for c in cs]
        grads = [
            ni[h] + fold(dot(v[...], s)) + totals(f_recv, g, c)
            for c, h, s in zip(cs, hs, ss_)
        ]
        outs = map_grads([k[...].T] * GG, [join(khl[h]) for h in hs], grads)
        for c, out in zip(cs, outs):
            odd = lax.rem(c, 2)
            sign = (1 - 2 * odd).astype(F32)
            own_half = jnp.where(even == (odd == 0), out * sign, 0.0)
            gk_sum[g, c // 2] += own_half

    gk_sum[...] = jnp.zeros_like(gk_sum)
    for g in range(NG):
        rotated(stage_g, g, GG)
        for p in range(PG // 2):
            gk_send[g, :, p] = gk_sum[g, p].reshape(NS, 8, DH)
        gk_recv[g, me] = gk_send[g, me]
        send_all(5, g, gk_send, gk_recv)

    def collect(phase, g, buf, out):
        def step(s, total):
            @pl.when(s != me)
            def _():
                arrived(phase, g, buf, s)

            return total + buf[g, s]

        total = lax.fori_loop(0, NS, step, jnp.zeros((PG // 2, 8, DH), F32))
        out[pl.ds(g * (PG // 2), PG // 2)] = total

    for g in range(NG):
        collect(4, g, gq_recv, oq)
    for g in range(NG):
        collect(5, g, gk_recv, ok)

    for phase, buf, dst_buf in (
        (0, a_send, a_recv),
        (1, c_send, c_recv),
        (2, d_send, d_recv),
        (3, f_send, f_recv),
        (4, gq_send, gq_recv),
        (5, gk_send, gk_recv),
    ):
        def drain(j, _, phase=phase, buf=buf, dst_buf=dst_buf):
            for g in range(NG):
                seq_copy(phase, g, buf, dst_buf, lax.rem(me + j, NS)).wait_send()
            return 0

        lax.fori_loop(1, NS, drain, 0)
    for j in range(1, NH):
        power_copy(lax.rem(hd + j, NH), hd).wait_send()


def unpack(pq, pk, oq, ok):
    for packed, out in ((pq, oq), (pk, ok)):
        for p in range(NS // 2):
            x = packed[p]
            out[2 * p] = x[:, :FH]
            out[2 * p + 1] = x[:, FH:]


def on_device(queries, keys, values, teacher, map_q, map_k):
    state = pltpu.VMEM((NG, NS, ROWS, DH), F32)
    share = pltpu.VMEM((NG, NS, PG // 2, 8, DH), F32)
    pair = pltpu.VMEM((NS, T, 2 * DH), BF16)
    whole = pltpu.VMEM((NS, T, DH), F32)
    vmem = pl.BlockSpec(memory_space=pltpu.VMEM)
    hbm = pl.BlockSpec(memory_space=pl.ANY)
    out = jax.ShapeDtypeStruct((NS // 2, 8, DH), F32)
    packed = pl.pallas_call(
        kernel,
        out_shape=(out, out),
        in_specs=[hbm] * 6,
        out_specs=(vmem, vmem),
        scratch_shapes=[
            pltpu.VMEM((T, NS * DH), BF16),
            pltpu.VMEM((T, NS * DH), BF16),
            pltpu.VMEM((NS, FH, DH), BF16),
            pltpu.VMEM((T, DH), BF16),
            pltpu.VMEM((T, DH), BF16),
            pltpu.VMEM((NS, FH, DH), BF16),
            pltpu.SemaphoreType.DMA((6,)),
            pair, pair, pair,
            whole, whole, whole,
            pltpu.VMEM((T, DH), F32),
            pltpu.VMEM((DH + 16, T), BF16),
            pltpu.VMEM((T, 2 * DH), BF16),
            pltpu.VMEM((2 * DH, DH), BF16),
            pltpu.VMEM((8, T), F32),
            pltpu.VMEM((NH, 8, T), F32),
            state, state, state, state, state, state, state, state,
            share, share, share, share,
            pltpu.VMEM((NG, PG // 2, DH, DH), F32),
            pltpu.SemaphoreType.DMA((6, NG, NS)),
            pltpu.SemaphoreType.DMA((6, NG, NS)),
            pltpu.SemaphoreType.DMA((NH,)),
            pltpu.SemaphoreType.DMA((NH,)),
        ],
        compiler_params=pltpu.CompilerParams(
            collective_id=0, has_side_effects=True, vmem_limit_bytes=56 * 2**20
        ),
    )(queries, keys, values, teacher, map_q.swapaxes(1, 2), map_k.swapaxes(1, 2))

    final = jax.ShapeDtypeStruct((NS, 8, FH), F32)
    return pl.pallas_call(unpack, out_shape=(final, final))(*packed)


def solution(mesh):
    placed = (
        P("seq", "head"),
        P("seq", "head"),
        P("seq", "head"),
        P("seq", "head"),
        P("head", None, None),
        P("head", None, None),
    )
    return jax.shard_map(
        on_device,
        mesh=mesh,
        in_specs=placed,
        out_specs=(P("head", "seq", None), P("head", "seq", None)),
        check_vma=False,
    )
```
